128 devices in a mesh: freq: 4 (over y), pts: 32 (over z, x, core).
Axes of the slice: x: 4, y: 4, z: 4, core: 2. Of those that a mesh axis runs over, the one named last changes fastest.
Arguments:
- data: float32 [2, 32, 64, 3, 32768], P(None, 'freq', None, None, 'pts'), may hold values from -180 to 180
- quad_weight: float32 [32768], P('pts'), may hold values from 0.2 to 5
- basis: float32 [2, 32, 64, 8], P(None, 'freq'), may hold values from -6 to 6
Outputs:
- basis_out: float32 [2, 32, 64, 8], P(None, 'freq')
- spectrum: float32 [32, 8], P('freq')
- modes: float32 [2, 32, 8, 3, 32768], P(None, 'freq', None, None, 'pts')
The draws below stay inside these ranges and needn't reach their ends.
All inputs are finite; a program needn't handle non-finite values.
Results may differ from the reference program's by a relative error of at most 0.0001.
Values sent between devices are 32-bit elements; how exact they have to be, the bound alone decides.
No kernel may reach another device: no remote copies, remote signals or barrier semaphores. Data moves between devices by JAX's collectives and lax.ppermute only.
A program may use at most 128 MiB of HBM per device.

```python
import math
import jax
import jax.numpy as jnp
from jax import lax

BLOCKS = 64
RANK = 8
COMP = 3
ITERS = 4
FREQ_ALL = 32
NPTS = 32768


def draw_data(key, part):
    first, second = jax.random.split(key, 2)
    shape = (2, FREQ_ALL, BLOCKS, COMP, NPTS)
    ramp = 1.0 + 2.0 * jnp.arange(FREQ_ALL, dtype=jnp.float32) / max(FREQ_ALL - 1, 1)
    block_scale = jnp.exp(jax.random.uniform(second, (FREQ_ALL, BLOCKS), jnp.float32, 0.0, math.log(10.0)))
    values = jnp.clip(jax.random.normal(first, shape, jnp.float32), -6.0, 6.0)
    scaled = values * (ramp[:, None] * block_scale)[None, :, :, None, None]
    return scaled.astype(jnp.float32)


def level_of(key, dims, pieces, smallest, high):
    factor_of = 1.0
    for axis_at, parts in pieces:
        heights = jax.random.uniform(jax.random.fold_in(jax.random.fold_in(key, 6), axis_at), (parts,), jnp.float32, smallest / len(pieces), high / len(pieces))
        factor_of = factor_of * jnp.repeat(jnp.exp(heights), dims[axis_at] // parts).reshape((-1,) + (1,) * (len(dims) - 1 - axis_at))
    return factor_of


def scatter_about(stream_key, dims, deviation, limit, shards=(), kind=jnp.bfloat16):
    gain = level_of(stream_key, dims, shards, -0.22, 0.18) if shards else 1.0
    result = jax.random.normal(stream_key, dims, jnp.float32) * deviation * gain
    return jnp.minimum(jnp.maximum(result, -limit), limit).astype(kind)


def setup_inputs(seed: int = 0) -> dict:
    keys = jax.random.split(jax.random.key(seed), 4)
    data = draw_data(jax.random.fold_in(keys[3], 71), 0)
    quad_weight = jnp.clip(jnp.exp(math.log(5.0) - 3.218876 * jax.random.uniform(keys[1], (NPTS,), jnp.float32) ** level_of(keys[1], (NPTS,), ((0, 32),), -0.2, 0.2)), 0.2, 5.0)
    basis = scatter_about(keys[2], (2, FREQ_ALL, BLOCKS, RANK), 1.0, 6.0, ((1, 4),), jnp.float32)
    return dict(data=data, quad_weight=quad_weight, basis=basis)


def matmul_high(left, right):
    return jnp.matmul(left, right, precision=lax.Precision.HIGHEST)

def apply_gram(gram_real, gram_imag, vec_real, vec_imag):
    out_real = matmul_high(gram_real, vec_real) - matmul_high(gram_imag, vec_imag)
    out_imag = matmul_high(gram_real, vec_imag) + matmul_high(gram_imag, vec_real)
    return (out_real, out_imag)

def orthonormalize(z_real, z_imag):
    blocks = z_real.shape[-2]
    cols_real = []
    cols_imag = []
    for column in range(z_real.shape[-1]):
        cur_real = z_real[..., column]
        cur_imag = z_imag[..., column]
        for earlier in range(column):
            base_real = cols_real[earlier]
            base_imag = cols_imag[earlier]
            coef_real = lax.optimization_barrier(jnp.sum(base_real * cur_real + base_imag * cur_imag, axis=-1)) / blocks
            coef_imag = lax.optimization_barrier(jnp.sum(base_real * cur_imag - base_imag * cur_real, axis=-1)) / blocks
            cur_real = cur_real - (coef_real[..., None] * base_real - coef_imag[..., None] * base_imag)
            cur_imag = cur_imag - (coef_real[..., None] * base_imag + coef_imag[..., None] * base_real)
        factor = lax.rsqrt(lax.optimization_barrier(jnp.mean(cur_real * cur_real + cur_imag * cur_imag, axis=-1)) + 1e-06)
        cols_real.append(cur_real * factor[..., None])
        cols_imag.append(cur_imag * factor[..., None])
    return (jnp.stack(cols_real, axis=-1), jnp.stack(cols_imag, axis=-1))

def reference(data, quad_weight, basis):
    scaling = 1.0 / (COMP * NPTS)
    weights = jnp.tile(quad_weight, COMP)

    def one_freq(index):
        block = lax.dynamic_index_in_dim(data, index, 1, keepdims=False)
        samples = block.reshape(2, BLOCKS, COMP * NPTS)
        weighted = samples * weights[None, None, :]
        gram_real = (matmul_high(samples[0], weighted[0].T) + matmul_high(samples[1], weighted[1].T)) * scaling
        gram_imag = (matmul_high(samples[0], weighted[1].T) - matmul_high(samples[1], weighted[0].T)) * scaling
        start = lax.dynamic_index_in_dim(basis, index, 1, keepdims=False)
        vec_real = start[0]
        vec_imag = start[1]
        for step in range(ITERS):
            z_real, z_imag = apply_gram(gram_real, gram_imag, vec_real, vec_imag)
            vec_real, vec_imag = orthonormalize(z_real, z_imag)
        z_real, z_imag = apply_gram(gram_real, gram_imag, vec_real, vec_imag)
        rayleigh = lax.optimization_barrier(jnp.sum(vec_real * z_real + vec_imag * z_imag, axis=-2)) / BLOCKS
        proj_real = matmul_high(vec_real.T, samples[0]) - matmul_high(vec_imag.T, samples[1])
        proj_imag = matmul_high(vec_imag.T, samples[0]) + matmul_high(vec_real.T, samples[1])
        projected = jnp.stack([proj_real, proj_imag]) / BLOCKS
        trace_value = jnp.sum(jnp.diagonal(gram_real))
        return (jnp.stack([vec_real, vec_imag]), rayleigh, projected.reshape(2, RANK, COMP, NPTS), trace_value)
    bases, rayleigh, projected, traces = lax.map(one_freq, jnp.arange(FREQ_ALL, dtype=jnp.int32))
    total = jnp.sum(traces)
    spectrum = rayleigh * (FREQ_ALL * BLOCKS) / total
    return (jnp.moveaxis(bases, 0, 1), spectrum, jnp.moveaxis(projected, 0, 1))
```

```python
import jax
import jax.numpy as jnp
from jax import lax
from jax.experimental import pallas as pl
from jax.experimental.pallas import tpu as pltpu
from jax.sharding import PartitionSpec as P

ITERS = 4
F32 = jnp.float32
BF16 = jnp.bfloat16


def split(x):
    high = x.astype(BF16)
    low = (x - high.astype(F32)).astype(BF16)
    return high, low


def dot_rows(left, right):
    return lax.dot_general(left, right, (((1,), (1,)), ((), ())), preferred_element_type=F32)


def dot_plain(left, right):
    return lax.dot_general(left, right, (((1,), (0,)), ((), ())), preferred_element_type=F32)


def gram_kernel(freqs, blocks, comps, scaling, data, weight, out, buf, sems):
    copies = [
        pltpu.make_async_copy(data.at[:, f], buf.at[f], sems.at[f]) for f in range(freqs)
    ]
    for copy in copies:
        copy.start()
    root = jnp.sqrt(weight[...])
    row = lax.broadcasted_iota(jnp.int32, (blocks, blocks), 0)
    col = lax.broadcasted_iota(jnp.int32, (blocks, blocks), 1)
    both = 2 * blocks
    trace = jnp.zeros((blocks, blocks), F32)
    for pair in range(freqs // 2):
        packed = []
        for f in (2 * pair, 2 * pair + 1):
            copies[f].wait()
            acc = jnp.zeros((both, 2 * both), F32)
            for c in range(comps):
                x = buf[f, :, c].reshape(both, -1) * root
                high, low = split(x)
                acc = acc + dot_rows(high, jnp.concatenate([high, low], axis=0))
            cross = acc[:, both:]
            full = (acc[:, :both] + (cross + cross.T)) * scaling
            real = full[:blocks, :blocks] + full[blocks:, blocks:]
            imag = full[:blocks, blocks:] - full[blocks:, :blocks]
            packed.append(jnp.where(row <= col, real, imag))
            trace = trace + jnp.where(row == col, real, 0.0)
        wide = jnp.concatenate(packed, axis=1)
        for b in range(blocks // 8):
            start = (pair * (blocks // 8) + b) * 9
            out[start : start + 8, 0, :] = wide[8 * b : 8 * b + 8, :]
    value = jnp.sum(jnp.sum(trace, axis=1, keepdims=True), axis=0, keepdims=True)
    line = jnp.broadcast_to(value, (1, both))
    for piece in range(freqs // 2 * blocks // 8):
        out[piece * 9 + 8, 0:1, :] = line


def sum_kernel(pieces, arrived, out, trace):
    total = arrived[0:8, 0, :]
    line = arrived[8, 0:1, :]
    for p in range(1, pieces):
        total = total + arrived[9 * p : 9 * p + 8, 0, :]
        line = line + arrived[9 * p + 8, 0:1, :]
    for p in range(pieces):
        out[p] = total
    trace[...] = line


def finish_kernel(freqs, blocks, comps, rank, gram, basis, data, vec_out, ray_out, modes, buf, res, sems, out_sems):
    reads = [pltpu.make_async_copy(data.at[:, f], buf.at[f], sems.at[f]) for f in range(freqs)]
    for copy in reads:
        copy.start()
    both = 2 * blocks
    row = lax.broadcasted_iota(jnp.int32, (blocks, blocks), 0)
    col = lax.broadcasted_iota(jnp.int32, (blocks, blocks), 1)
    mats = []
    for f in range(freqs):
        packed = gram[f // 2][:, (f % 2) * blocks : (f % 2 + 1) * blocks]
        flipped = packed.T
        real = jnp.where(row <= col, packed, flipped)
        imag = jnp.where(row > col, packed, jnp.where(row < col, -flipped, 0.0))
        top = jnp.concatenate([real, -imag], axis=1)
        bottom = jnp.concatenate([imag, real], axis=1)
        high, low = split(jnp.concatenate([top, bottom], axis=0))
        mats.append(jnp.concatenate([high, low], axis=1))

    def apply(vec):
        parts = []
        for f in range(freqs):
            high, low = split(vec[f])
            out = dot_plain(jnp.concatenate([high, low], axis=0), mats[f])
            out = out[:rank] + out[rank:]
            parts.append((out[:, both:] + out[:, :both])[None])
        return jnp.concatenate(parts, axis=0)

    lane = lax.broadcasted_iota(jnp.int32, (1, 1, both), 2)
    sub = lax.broadcasted_iota(jnp.int32, (1, rank, 1), 1)
    sign = jnp.where(lane < blocks, -1.0, 1.0).astype(F32)

    def orthonormalize(z):
        for k in range(rank):
            base = z[:, k : k + 1, :]
            turned = pltpu.roll(base.reshape(freqs, both), blocks, 1).reshape(freqs, 1, both) * sign
            norm = jnp.sum(base * base, axis=2, keepdims=True) * (1.0 / blocks) + 1e-6
            factor = lax.rsqrt(norm)
            if k + 1 < rank:
                dot_real = jnp.sum(base * z, axis=2, keepdims=True)
                dot_imag = jnp.sum(turned * z, axis=2, keepdims=True)
                square = factor * factor * (1.0 / blocks)
                moved = z - (dot_real * square) * base - (dot_imag * square) * turned
            else:
                moved = z
            z = jnp.where(sub == k, z * factor, jnp.where(sub > k, moved, z))
        return z

    vec = jnp.concatenate([basis[0], basis[1]], axis=2)
    for step in range(ITERS):
        vec = orthonormalize(apply(vec))
    z = apply(vec)
    ray = jnp.sum(vec * z, axis=2, keepdims=True) * (1.0 / blocks)
    ray_out[...] = jnp.sum(jnp.where(sub == lane, ray, 0.0), axis=1)[:, :rank]
    vec_out[0] = vec[:, :, :blocks]
    vec_out[1] = vec[:, :, blocks:]

    writes = []
    for f in range(freqs):
        reads[f].wait()
        v = vec[f] * (1.0 / blocks)
        real_row = jnp.where(lane[0] < blocks, v, -v)
        imag_row = pltpu.roll(v, blocks, 1)
        high, low = split(jnp.concatenate([real_row, imag_row], axis=0))
        coef = jnp.concatenate(
            [jnp.concatenate([high, high], axis=1), jnp.concatenate([low, jnp.zeros_like(low)], axis=1)], axis=0
        )
        for c in range(comps):
            x = buf[f, :, c].reshape(both, -1)
            x_high, x_low = split(x)
            out = dot_plain(coef, jnp.concatenate([x_high, x_low], axis=0))
            out = out[: 2 * rank] + out[2 * rank :]
            res[0, f, c] = out[:rank]
            res[1, f, c] = out[rank:]
        copy = pltpu.make_async_copy(res.at[:, f], modes.at[:, f], out_sems.at[f])
        copy.start()
        writes.append(copy)
    for copy in writes:
        copy.wait()


def per_device(data, quad_weight, basis):
    _, freqs, blocks, comps, points = data.shape
    rank = basis.shape[-1]
    freq_groups = lax.axis_size("freq")
    size = lax.axis_size("pts")
    freq_count = freqs * freq_groups
    scaling = 1.0 / (comps * points * size)
    pieces = freqs // 2 * blocks // 8
    samples = jnp.transpose(data, (0, 1, 3, 2, 4))
    start = jnp.transpose(basis, (0, 1, 3, 2))
    vmem = pl.BlockSpec(memory_space=pltpu.VMEM)
    hbm = pl.BlockSpec(memory_space=pltpu.MemorySpace.HBM)
    packed = pl.pallas_call(
        lambda *refs: gram_kernel(freqs, blocks, comps, scaling, *refs),
        out_shape=jax.ShapeDtypeStruct((pieces * 9, 1, 2 * blocks), F32),
        in_specs=[hbm, vmem],
        out_specs=vmem,
        scratch_shapes=[
            pltpu.VMEM((freqs, 2, comps, blocks, points), F32),
            pltpu.SemaphoreType.DMA((freqs,)),
        ],
        compiler_params=pltpu.CompilerParams(vmem_limit_bytes=60 * 2**20),
        name="gram",
    )(samples, quad_weight.reshape(1, points))
    arrived = lax.all_to_all(packed, "pts", 0, 0, tiled=True)
    spread, trace = pl.pallas_call(
        lambda *refs: sum_kernel(size, *refs),
        out_shape=(
            jax.ShapeDtypeStruct((size, 8, 2 * blocks), F32),
            jax.ShapeDtypeStruct((1, 2 * blocks), F32),
        ),
        in_specs=[vmem],
        out_specs=(vmem, vmem),
        compiler_params=pltpu.CompilerParams(vmem_limit_bytes=2 * 2**20),
        name="total",
    )(arrived)
    trace = trace + lax.ppermute(trace, "freq", [(i, i ^ 1) for i in range(freq_groups)])
    gram = lax.all_to_all(spread, "pts", 0, 0, tiled=True).reshape(freqs // 2, blocks, 2 * blocks)
    gram, trace = lax.optimization_barrier((gram, trace))
    other = lax.ppermute(trace, "freq", [(i, i ^ 2) for i in range(freq_groups)])
    vec, ray, modes = pl.pallas_call(
        lambda *refs: finish_kernel(freqs, blocks, comps, rank, *refs),
        out_shape=(
            jax.ShapeDtypeStruct((2, freqs, rank, blocks), F32),
            jax.ShapeDtypeStruct((freqs, rank), F32),
            jax.ShapeDtypeStruct((2, freqs, comps, rank, points), F32),
        ),
        in_specs=[vmem, vmem, hbm],
        out_specs=(vmem, vmem, hbm),
        scratch_shapes=[
            pltpu.VMEM((freqs, 2, comps, blocks, points), F32),
            pltpu.VMEM((2, freqs, comps, rank, points), F32),
            pltpu.SemaphoreType.DMA((freqs,)),
            pltpu.SemaphoreType.DMA((freqs,)),
        ],
        compiler_params=pltpu.CompilerParams(vmem_limit_bytes=60 * 2**20),
        name="finish",
    )(gram, start, samples)
    total = (trace + other)[0, 0]
    spectrum = ray * (freq_count * blocks) / total
    return (
        jnp.transpose(vec, (0, 1, 3, 2)),
        spectrum,
        jnp.transpose(modes, (0, 1, 3, 2, 4)),
    )


def solution(mesh):
    in_specs = (P(None, "freq", None, None, "pts"), P("pts"), P(None, "freq", None, None))
    out_specs = (P(None, "freq", None, None), P("freq", None), P(None, "freq", None, None, "pts"))
    return jax.shard_map(
        per_device, mesh=mesh, in_specs=in_specs, out_specs=out_specs, check_vma=False
    )
```

```python
import jax
import jax.numpy as jnp
from jax import lax
from jax.experimental import pallas as pl
from jax.experimental.pallas import tpu as pltpu
from jax.sharding import PartitionSpec as P

ITERS = 4
F32 = jnp.float32
BF16 = jnp.bfloat16


def split(x):
    high = x.astype(BF16)
    low = (x - high.astype(F32)).astype(BF16)
    return high, low


def dot_plain(left, right):
    return lax.dot_general(left, right, (((1,), (0,)), ((), ())), preferred_element_type=F32)


def gram_kernel(freqs, blocks, comps, scaling, data, weight, out, buf, lines, sums, sems):
    def read(f):
        return pltpu.make_async_copy(data.at[:, f], buf.at[f], sems.at[f])

    weight_read = pltpu.make_async_copy(weight, lines, sems.at[freqs])
    weight_read.start()
    for f in range(freqs):
        read(f).start()
    weight_read.wait()
    root = jnp.sqrt(lines[...])
    row = lax.broadcasted_iota(jnp.int32, (blocks, blocks), 0)
    col = lax.broadcasted_iota(jnp.int32, (blocks, blocks), 1)
    both = 2 * blocks

    def multiply(pair):
        for half in range(2):
            read(2 * pair + half).wait()
        for half in range(2):
            f = 2 * pair + half
            acc = jnp.zeros((both, 2 * both), F32)
            for c in range(comps):
                x = buf[f, :, c].reshape(both, -1) * root
                high, low = split(x)
                acc = acc + dot_plain(high, jnp.concatenate([high.T, low.T], axis=1))
            sums[f] = acc

    def pack(pair, trace):
        packed = []
        for half in range(2):
            acc = sums[2 * pair + half]
            cross = acc[:, both:]
            full = (acc[:, :both] + (cross + cross.T)) * scaling
            real = full[:blocks, :blocks] + full[blocks:, blocks:]
            imag = full[:blocks, blocks:] - full[blocks:, :blocks]
            packed.append(jnp.where(row <= col, real, imag))
            trace = trace + jnp.where(row == col, real, 0.0)
        wide = jnp.concatenate(packed, axis=1)
        for b in range(blocks // 8):
            start = (pair * (blocks // 8) + b) * 9
            out[pl.ds(start, 8), 0, :] = wide[8 * b : 8 * b + 8, :]
        return trace

    def pair_step(pair, trace):
        trace = pack(pair - 1, trace)
        multiply(pair)
        return trace

    pairs = freqs // 2
    multiply(0)
    trace = lax.fori_loop(1, pairs, pair_step, jnp.zeros((blocks, blocks), F32))
    trace = pack(pairs - 1, trace)
    value = jnp.sum(jnp.sum(trace, axis=1, keepdims=True), axis=0, keepdims=True)
    line = jnp.broadcast_to(value, (1, both))
    for piece in range(freqs // 2 * blocks // 8):
        out[piece * 9 + 8, 0:1, :] = line


def sum_kernel(pieces, arrived, out, trace):
    total = arrived[0:8, 0, :]
    line = arrived[8, 0:1, :]
    for p in range(1, pieces):
        total = total + arrived[9 * p : 9 * p + 8, 0, :]
        line = line + arrived[9 * p + 8, 0:1, :]
    for p in range(pieces):
        out[p] = total
    trace[...] = line


def finish_kernel(freqs, blocks, comps, rank, gram, basis, data, vec_out, ray_out, modes, buf, res, vecs, mats, coefs, sems, out_sems):
    def read(f):
        return pltpu.make_async_copy(data.at[:, f], buf.at[f], sems.at[f])

    def write(f):
        return pltpu.make_async_copy(res.at[:, f], modes.at[:, f], out_sems.at[f])

    for f in range(freqs):
        read(f).start()
    both = 2 * blocks
    row = lax.broadcasted_iota(jnp.int32, (blocks, blocks), 0)
    col = lax.broadcasted_iota(jnp.int32, (blocks, blocks), 1)
    for f in range(freqs):
        packed = gram[f // 2][:, (f % 2) * blocks : (f % 2 + 1) * blocks]
        flipped = packed.T
        real = jnp.where(row <= col, packed, flipped)
        imag = jnp.where(row > col, packed, jnp.where(row < col, -flipped, 0.0))
        top = jnp.concatenate([real, -imag], axis=1)
        bottom = jnp.concatenate([imag, real], axis=1)
        high, low = split(jnp.concatenate([top, bottom], axis=0))
        mats[f] = jnp.concatenate([high, low], axis=1)

    def apply(vec):
        parts = []
        for f in range(freqs):
            high, low = split(vec[f])
            out = dot_plain(jnp.concatenate([high, low], axis=0), mats[f])
            out = out[:rank] + out[rank:]
            parts.append((out[:, both:] + out[:, :both])[None])
        return jnp.concatenate(parts, axis=0)

    lane = lax.broadcasted_iota(jnp.int32, (1, 1, both), 2)
    sub = lax.broadcasted_iota(jnp.int32, (1, rank, 1), 1)
    sign = jnp.where(lane < blocks, -1.0, 1.0).astype(F32)

    def orthonormalize(z):
        turned = pltpu.roll(z.reshape(freqs * rank, both), blocks, 1).reshape(z.shape) * sign
        for k in range(rank):
            base = z[:, k : k + 1, :]
            across = turned[:, k : k + 1, :]
            dot_real = jnp.sum(base * z, axis=2, keepdims=True)
            norm = dot_real[:, k : k + 1, :] * (1.0 / blocks) + 1e-6
            factor = lax.rsqrt(norm)
            if k + 1 < rank:
                dot_imag = jnp.sum(across * z, axis=2, keepdims=True)
                square = factor * factor * (1.0 / blocks)
                low = jnp.where(sub > k, square, 0.0)
                keep = jnp.where(sub == k, factor, 1.0)
                coef_real = dot_real * low
                coef_imag = dot_imag * low
                z, turned = (
                    z * keep - coef_real * base - coef_imag * across,
                    turned * keep - coef_real * across + coef_imag * base,
                )
            else:
                z = jnp.where(sub == k, z * factor, z)
        return z

    vec = jnp.concatenate([basis[0], basis[1]], axis=2)
    vec = lax.fori_loop(0, ITERS, lambda step, v: orthonormalize(apply(v)), vec)
    z = apply(vec)
    ray = jnp.sum(vec * z, axis=2, keepdims=True) * (1.0 / blocks)
    ray_out[...] = jnp.sum(jnp.where(sub == lane, ray, 0.0), axis=1)[:, :rank]
    vecs[0] = vec[:, :, :blocks]
    vecs[1] = vec[:, :, blocks:]
    vec_write = pltpu.make_async_copy(vecs, vec_out, out_sems.at[freqs])
    vec_write.start()
    for f in range(freqs):
        v = vec[f] * (1.0 / blocks)
        real_row = jnp.where(lane[0] < blocks, v, -v)
        imag_row = pltpu.roll(v, blocks, 1)
        high, low = split(jnp.concatenate([real_row, imag_row], axis=0))
        coefs[f] = jnp.concatenate(
            [jnp.concatenate([high, high], axis=1), jnp.concatenate([low, jnp.zeros_like(low)], axis=1)], axis=0
        )

    def project(f, carry):
        read(f).wait()
        coef = coefs[f]
        for c in range(comps):
            x = buf[f, :, c].reshape(both, -1)
            x_high, x_low = split(x)
            out = dot_plain(coef, jnp.concatenate([x_high, x_low], axis=0))
            out = out[: 2 * rank] + out[2 * rank :]
            res[0, f, c] = out[:rank]
            res[1, f, c] = out[rank:]
        write(f).start()
        return carry

    lax.fori_loop(0, freqs, project, 0)
    for f in range(freqs):
        write(f).wait()
    vec_write.wait()


def program(data, quad_weight, basis):
    _, freqs, blocks, comps, points = data.shape
    rank = basis.shape[-1]
    freq_groups = lax.axis_size("freq")
    size = lax.axis_size("pts")
    freq_count = freqs * freq_groups
    scaling = 1.0 / (comps * points * size)
    pieces = freqs // 2 * blocks // 8
    samples = jnp.transpose(data, (0, 1, 3, 2, 4))
    start = jnp.transpose(basis, (0, 1, 3, 2))
    vmem = pl.BlockSpec(memory_space=pltpu.VMEM)
    hbm = pl.BlockSpec(memory_space=pltpu.MemorySpace.HBM)
    packed = pl.pallas_call(
        lambda *refs: gram_kernel(freqs, blocks, comps, scaling, *refs),
        out_shape=pltpu.VMEM((pieces * 9, 1, 2 * blocks), F32),
        in_specs=[hbm, hbm],
        out_specs=vmem,
        scratch_shapes=[
            pltpu.VMEM((freqs, 2, comps, blocks, points), F32),
            pltpu.VMEM((1, points), F32),
            pltpu.VMEM((freqs, 2 * blocks, 4 * blocks), F32),
            pltpu.SemaphoreType.DMA((freqs + 1,)),
        ],
        compiler_params=pltpu.CompilerParams(vmem_limit_bytes=60 * 2**20),
        name="gram",
    )(samples, quad_weight.reshape(1, points))
    arrived = lax.all_to_all(packed, "pts", 0, 0, tiled=True)
    spread, trace = pl.pallas_call(
        lambda *refs: sum_kernel(size, *refs),
        out_shape=(
            jax.ShapeDtypeStruct((size, 8, 2 * blocks), F32),
            jax.ShapeDtypeStruct((1, 2 * blocks), F32),
        ),
        in_specs=[vmem],
        out_specs=(vmem, vmem),
        compiler_params=pltpu.CompilerParams(vmem_limit_bytes=2 * 2**20),
        name="total",
    )(arrived)
    trace = trace + lax.ppermute(trace, "freq", [(i, i ^ 1) for i in range(freq_groups)])
    gram = lax.all_to_all(spread, "pts", 0, 0, tiled=True).reshape(freqs // 2, blocks, 2 * blocks)
    other = lax.ppermute(trace, "freq", [(i, freq_groups - 1 - i) for i in range(freq_groups)])
    vec, ray, modes = pl.pallas_call(
        lambda *refs: finish_kernel(freqs, blocks, comps, rank, *refs),
        out_shape=(
            jax.ShapeDtypeStruct((2, freqs, rank, blocks), F32),
            pltpu.VMEM((freqs, rank), F32),
            jax.ShapeDtypeStruct((2, freqs, comps, rank, points), F32),
        ),
        in_specs=[vmem, vmem, hbm],
        out_specs=(hbm, vmem, hbm),
        scratch_shapes=[
            pltpu.VMEM((freqs, 2, comps, blocks, points), F32),
            pltpu.VMEM((2, freqs, comps, rank, points), F32),
            pltpu.VMEM((2, freqs, rank, blocks), F32),
            pltpu.VMEM((freqs, 2 * blocks, 4 * blocks), BF16),
            pltpu.VMEM((freqs, 4 * rank, 4 * blocks), BF16),
            pltpu.SemaphoreType.DMA((freqs,)),
            pltpu.SemaphoreType.DMA((freqs + 1,)),
        ],
        compiler_params=pltpu.CompilerParams(vmem_limit_bytes=52 * 2**20),
        name="finish",
    )(gram, start, samples)
    total = (trace + other)[0, 0]
    spectrum = ray * (freq_count * blocks) / total
    return (
        jnp.transpose(vec, (0, 1, 3, 2)),
        spectrum,
        jnp.transpose(modes, (0, 1, 3, 2, 4)),
    )


def solution(mesh):
    in_specs = (P(None, "freq", None, None, "pts"), P("pts"), P(None, "freq", None, None))
    out_specs = (P(None, "freq", None, None), P("freq", None), P(None, "freq", None, None, "pts"))
    return jax.shard_map(
        program, mesh=mesh, in_specs=in_specs, out_specs=out_specs, check_vma=False
    )
```

```python
import jax
import jax.numpy as jnp
from jax import lax
from jax.experimental import pallas as pl
from jax.experimental.pallas import tpu as pltpu
from jax.sharding import PartitionSpec as P

ITERS = 4
TOGETHER = 4
F32 = jnp.float32
BF16 = jnp.bfloat16


def split(x):
    high = x.astype(BF16)
    low = (x - high.astype(F32)).astype(BF16)
    return high, low


def dot_rows(left, right):
    return lax.dot_general(left, right, (((1,), (1,)), ((), ())), preferred_element_type=F32)


def dot_plain(left, right):
    return lax.dot_general(left, right, (((1,), (0,)), ((), ())), preferred_element_type=F32)


def gram_kernel(freqs, blocks, comps, scaling, data, weight, out, buf, lines, sums, sems):
    def read(f):
        return pltpu.make_async_copy(data.at[:, f], buf.at[f], sems.at[f])

    weight_read = pltpu.make_async_copy(weight, lines, sems.at[freqs])
    weight_read.start()
    for f in range(freqs):
        read(f).start()
    weight_read.wait()
    root = jnp.sqrt(lines[...])
    row = lax.broadcasted_iota(jnp.int32, (blocks, blocks), 0)
    col = lax.broadcasted_iota(jnp.int32, (blocks, blocks), 1)
    both = 2 * blocks

    def multiply(first, count):
        for f in range(count):
            read(first + f).wait()
        for f in range(count):
            f = first + f
            acc = jnp.zeros((both, 2 * both), F32)
            for c in range(comps):
                x = buf[f, :, c].reshape(both, -1) * root
                high, low = split(x)
                acc = acc + dot_plain(high, jnp.concatenate([high.T, low.T], axis=1))
            sums[f] = acc

    def pack(pair, trace):
        packed = []
        for half in range(2):
            acc = sums[2 * pair + half]
            cross = acc[:, both:]
            full = (acc[:, :both] + (cross + cross.T)) * scaling
            real = full[:blocks, :blocks] + full[blocks:, blocks:]
            imag = full[:blocks, blocks:] - full[blocks:, :blocks]
            packed.append(jnp.where(row <= col, real, imag))
            trace = trace + jnp.where(row == col, real, 0.0)
        wide = jnp.concatenate(packed, axis=1)
        for b in range(blocks // 8):
            start = (pair * (blocks // 8) + b) * 9
            out[pl.ds(start, 8), 0, :] = wide[8 * b : 8 * b + 8, :]
        return trace

    def pair_step(pair, trace):
        trace = pack(pair - 1, trace)
        multiply(2 * pair, 2)
        return trace

    pairs = freqs // 2
    multiply(0, 1)
    multiply(1, 1)
    trace = jnp.zeros((blocks, blocks), F32)
    for pair in range(1, pairs):
        trace = pair_step(pair, trace)
    trace = pack(pairs - 1, trace)
    value = jnp.sum(jnp.sum(trace, axis=1, keepdims=True), axis=0, keepdims=True)
    line = jnp.broadcast_to(value, (1, both))
    for piece in range(freqs // 2 * blocks // 8):
        out[piece * 9 + 8, 0:1, :] = line


def sum_kernel(pieces, arrived, out, trace):
    total = arrived[0:8, 0, :]
    line = arrived[8, 0:1, :]
    for p in range(1, pieces):
        total = total + arrived[9 * p : 9 * p + 8, 0, :]
        line = line + arrived[9 * p + 8, 0:1, :]
    for p in range(pieces):
        out[p] = total
    trace[...] = line


def finish_kernel(freqs, blocks, comps, rank, groups, gram, basis, data, *refs):
    traces = refs[:groups]
    vec_out, spectrum, modes, buf, res, vecs, rates, mats, coefs, sems, out_sems = refs[groups:]

    def read(f):
        return pltpu.make_async_copy(data.at[:, f], buf.at[f], sems.at[f])

    def write(f):
        return pltpu.make_async_copy(res.at[:, f], modes.at[:, f], out_sems.at[f])

    for f in range(freqs):
        read(f).start()
    both = 2 * blocks
    row = lax.broadcasted_iota(jnp.int32, (blocks, blocks), 0)
    col = lax.broadcasted_iota(jnp.int32, (blocks, blocks), 1)
    for f in range(freqs):
        packed = gram[f // 2][:, (f % 2) * blocks : (f % 2 + 1) * blocks]
        flipped = packed.T
        real = jnp.where(row <= col, packed, flipped)
        imag = jnp.where(row > col, packed, jnp.where(row < col, -flipped, 0.0))
        top = jnp.concatenate([real, -imag], axis=1)
        bottom = jnp.concatenate([imag, real], axis=1)
        high, low = split(jnp.concatenate([top, bottom], axis=0))
        mats[f] = jnp.concatenate([high, low], axis=1)

    def apply(vec):
        parts = []
        for f in range(freqs):
            high, low = split(vec[f])
            out = dot_plain(jnp.concatenate([high, low], axis=0), mats[f])
            out = out[:rank] + out[rank:]
            parts.append((out[:, both:] + out[:, :both])[None])
        return jnp.concatenate(parts, axis=0)

    lane = lax.broadcasted_iota(jnp.int32, (1, 1, both), 2)
    sub = lax.broadcasted_iota(jnp.int32, (1, rank, 1), 1)
    sign = jnp.where(lane < blocks, -1.0, 1.0).astype(F32)

    def orthonormalize(z):
        turned = pltpu.roll(z.reshape(freqs * rank, both), blocks, 1).reshape(z.shape) * sign
        for k in range(rank):
            base = z[:, k : k + 1, :]
            across = turned[:, k : k + 1, :]
            dot_real = jnp.sum(base * z, axis=2, keepdims=True)
            norm = dot_real[:, k : k + 1, :] * (1.0 / blocks) + 1e-6
            factor = lax.rsqrt(norm)
            if k + 1 < rank:
                dot_imag = jnp.sum(across * z, axis=2, keepdims=True)
                square = factor * factor * (1.0 / blocks)
                low = jnp.where(sub > k, square, 0.0)
                keep = jnp.where(sub == k, factor, 1.0)
                coef_real = dot_real * low
                coef_imag = dot_imag * low
                z, turned = (
                    z * keep - coef_real * base - coef_imag * across,
                    turned * keep - coef_real * across + coef_imag * base,
                )
            else:
                z = jnp.where(sub == k, z * factor, z)
        return z

    vec = jnp.concatenate([basis[0], basis[1]], axis=2)
    for step in range(ITERS):
        vec = orthonormalize(apply(vec))
    z = apply(vec)
    ray = jnp.sum(vec * z, axis=2, keepdims=True) * (1.0 / blocks)
    total = traces[0][...]
    for line in traces[1:]:
        total = total + line[...]
    energy = jnp.sum(jnp.where(sub == lane, ray, 0.0), axis=1) * (freqs * groups * blocks)
    rates[...] = (energy / total)[:, :rank]
    rate_write = pltpu.make_async_copy(rates, spectrum, out_sems.at[freqs + 1])
    rate_write.start()
    vecs[0] = vec[:, :, :blocks]
    vecs[1] = vec[:, :, blocks:]
    vec_write = pltpu.make_async_copy(vecs, vec_out, out_sems.at[freqs])
    vec_write.start()
    for f in range(freqs):
        v = vec[f] * (1.0 / blocks)
        real_row = jnp.where(lane[0] < blocks, v, -v)
        imag_row = pltpu.roll(v, blocks, 1)
        high, low = split(jnp.concatenate([real_row, imag_row], axis=0))
        coefs[f] = jnp.concatenate(
            [jnp.concatenate([high, high], axis=1), jnp.concatenate([low, jnp.zeros_like(low)], axis=1)], axis=0
        )

    def project(step, carry):
        first = step * TOGETHER
        for f in range(TOGETHER):
            read(first + f).wait()
        for f in range(TOGETHER):
            f = first + f
            coef = coefs[f]
            for c in range(comps):
                x = buf[f, :, c].reshape(both, -1)
                x_high, x_low = split(x)
                out = dot_plain(coef, jnp.concatenate([x_high, x_low], axis=0))
                out = out[: 2 * rank] + out[2 * rank :]
                res[0, f, c] = out[:rank]
                res[1, f, c] = out[rank:]
            write(f).start()
        return carry

    lax.fori_loop(0, freqs // TOGETHER, project, 0)
    for f in range(freqs):
        write(f).wait()
    vec_write.wait()
    rate_write.wait()


def per_device(data, quad_weight, basis):
    _, freqs, blocks, comps, points = data.shape
    rank = basis.shape[-1]
    freq_groups = lax.axis_size("freq")
    size = lax.axis_size("pts")
    freq_count = freqs * freq_groups
    scaling = 1.0 / (comps * points * size)
    pieces = freqs // 2 * blocks // 8
    samples = jnp.transpose(data, (0, 1, 3, 2, 4))
    start = jnp.transpose(basis, (0, 1, 3, 2))
    vmem = pl.BlockSpec(memory_space=pltpu.VMEM)
    hbm = pl.BlockSpec(memory_space=pltpu.MemorySpace.HBM)
    packed = pl.pallas_call(
        lambda *refs: gram_kernel(freqs, blocks, comps, scaling, *refs),
        out_shape=pltpu.VMEM((pieces * 9, 1, 2 * blocks), F32),
        in_specs=[hbm, hbm],
        out_specs=vmem,
        scratch_shapes=[
            pltpu.VMEM((freqs, 2, comps, blocks, points), F32),
            pltpu.VMEM((1, points), F32),
            pltpu.VMEM((freqs, 2 * blocks, 4 * blocks), F32),
            pltpu.SemaphoreType.DMA((freqs + 1,)),
        ],
        compiler_params=pltpu.CompilerParams(vmem_limit_bytes=60 * 2**20),
        name="gram",
    )(samples, quad_weight.reshape(1, points))
    arrived = lax.all_to_all(packed, "pts", 0, 0, tiled=True)
    spread, trace = pl.pallas_call(
        lambda *refs: sum_kernel(size, *refs),
        out_shape=(
            jax.ShapeDtypeStruct((size, 8, 2 * blocks), F32),
            jax.ShapeDtypeStruct((1, 2 * blocks), F32),
        ),
        in_specs=[vmem],
        out_specs=(vmem, vmem),
        compiler_params=pltpu.CompilerParams(vmem_limit_bytes=2 * 2**20),
        name="total",
    )(arrived)
    others = [
        lax.ppermute(trace, "freq", [(i, (i + d) % freq_groups) for i in range(freq_groups)])
        for d in range(1, freq_groups)
    ]
    gram = lax.all_to_all(spread, "pts", 0, 0, tiled=True).reshape(freqs // 2, blocks, 2 * blocks)
    traces = [trace, *others]
    vec, spectrum, modes = pl.pallas_call(
        lambda *refs: finish_kernel(freqs, blocks, comps, rank, freq_groups, *refs),
        out_shape=(
            jax.ShapeDtypeStruct((2, freqs, rank, blocks), F32),
            jax.ShapeDtypeStruct((freqs, rank), F32),
            jax.ShapeDtypeStruct((2, freqs, comps, rank, points), F32),
        ),
        in_specs=[vmem, vmem, hbm] + [vmem] * freq_groups,
        out_specs=(hbm, hbm, hbm),
        scratch_shapes=[
            pltpu.VMEM((freqs, 2, comps, blocks, points), F32),
            pltpu.VMEM((2, freqs, comps, rank, points), F32),
            pltpu.VMEM((2, freqs, rank, blocks), F32),
            pltpu.VMEM((freqs, rank), F32),
            pltpu.VMEM((freqs, 2 * blocks, 4 * blocks), BF16),
            pltpu.VMEM((freqs, 4 * rank, 4 * blocks), BF16),
            pltpu.SemaphoreType.DMA((freqs,)),
            pltpu.SemaphoreType.DMA((freqs + 2,)),
        ],
        compiler_params=pltpu.CompilerParams(vmem_limit_bytes=52 * 2**20),
        name="finish",
    )(gram, start, samples, *traces)
    return (
        jnp.transpose(vec, (0, 1, 3, 2)),
        spectrum,
        jnp.transpose(modes, (0, 1, 3, 2, 4)),
    )


def solution(mesh):
    in_specs = (P(None, "freq", None, None, "pts"), P("pts"), P(None, "freq", None, None))
    out_specs = (P(None, "freq", None, None), P("freq", None), P(None, "freq", None, None, "pts"))
    return jax.shard_map(
        per_device, mesh=mesh, in_specs=in_specs, out_specs=out_specs, check_vma=False
    )
```

```python
import jax
import jax.numpy as jnp
from jax import lax
from jax.experimental import pallas as pl
from jax.experimental.pallas import tpu as pltpu
from jax.sharding import PartitionSpec as P

ITERS = 4
TOGETHER = 4
F32 = jnp.float32
BF16 = jnp.bfloat16


def split(x):
    high = x.astype(BF16)
    low = (x - high.astype(F32)).astype(BF16)
    return high, low


def dot_rows(left, right):
    return lax.dot_general(left, right, (((1,), (1,)), ((), ())), preferred_element_type=F32)


def dot_plain(left, right):
    return lax.dot_general(left, right, (((1,), (0,)), ((), ())), preferred_element_type=F32)


def gram_kernel(freqs, blocks, comps, scaling, data, weight, out, buf, lines, sums, sems):
    def read(f):
        return pltpu.make_async_copy(data.at[:, f], buf.at[f], sems.at[f])

    def read_first(c):
        return pltpu.make_async_copy(data.at[:, 0, c], buf.at[0, :, c], sems.at[freqs + 1 + c])

    weight_read = pltpu.make_async_copy(weight, lines, sems.at[freqs])
    weight_read.start()
    for c in range(comps):
        read_first(c).start()
    for f in range(1, freqs):
        read(f).start()
    weight_read.wait()
    root = jnp.sqrt(lines[...])
    row = lax.broadcasted_iota(jnp.int32, (blocks, blocks), 0)
    col = lax.broadcasted_iota(jnp.int32, (blocks, blocks), 1)
    both = 2 * blocks

    def product(f, c):
        x = buf[f, :, c].reshape(both, -1) * root
        high, low = split(x)
        return dot_plain(high, jnp.concatenate([high.T, low.T], axis=1))

    def multiply(first, count):
        for f in range(count):
            read(first + f).wait()
        for f in range(first, first + count):
            acc = jnp.zeros((both, 2 * both), F32)
            for c in range(comps):
                acc = acc + product(f, c)
            sums[f] = acc

    def pack(pair, trace):
        packed = []
        for half in range(2):
            acc = sums[2 * pair + half]
            cross = acc[:, both:]
            full = (acc[:, :both] + (cross + cross.T)) * scaling
            real = full[:blocks, :blocks] + full[blocks:, blocks:]
            imag = full[:blocks, blocks:] - full[blocks:, :blocks]
            packed.append(jnp.where(row <= col, real, imag))
            trace = trace + jnp.where(row == col, real, 0.0)
        wide = jnp.concatenate(packed, axis=1)
        for b in range(blocks // 8):
            start = (pair * (blocks // 8) + b) * 9
            out[pl.ds(start, 8), 0, :] = wide[8 * b : 8 * b + 8, :]
        return trace

    def pair_step(pair, trace):
        trace = pack(pair - 1, trace)
        multiply(2 * pair, 2)
        return trace

    pairs = freqs // 2
    acc = jnp.zeros((both, 2 * both), F32)
    for c in range(comps):
        read_first(c).wait()
        acc = acc + product(0, c)
    sums[0] = acc
    multiply(1, 1)
    trace = jnp.zeros((blocks, blocks), F32)
    for pair in range(1, pairs):
        trace = pair_step(pair, trace)
    trace = pack(pairs - 1, trace)
    value = jnp.sum(jnp.sum(trace, axis=1, keepdims=True), axis=0, keepdims=True)
    line = jnp.broadcast_to(value, (1, both))
    for piece in range(freqs // 2 * blocks // 8):
        out[piece * 9 + 8, 0:1, :] = line


def sum_kernel(pieces, arrived, out, trace):
    total = arrived[0:8, 0, :]
    line = arrived[8, 0:1, :]
    for p in range(1, pieces):
        total = total + arrived[9 * p : 9 * p + 8, 0, :]
        line = line + arrived[9 * p + 8, 0:1, :]
    for p in range(pieces):
        out[p] = total
    trace[...] = line


def finish_kernel(freqs, blocks, comps, rank, groups, gram, basis, data, *refs):
    traces = refs[:groups]
    vec_out, spectrum, modes, buf, res, vecs, rates, mats, coefs, sems, out_sems = refs[groups:]

    def read(f):
        return pltpu.make_async_copy(data.at[:, f], buf.at[f], sems.at[f])

    def write(f):
        return pltpu.make_async_copy(res.at[:, f], modes.at[:, f], out_sems.at[f])

    for f in range(freqs):
        read(f).start()
    both = 2 * blocks
    row = lax.broadcasted_iota(jnp.int32, (blocks, blocks), 0)
    col = lax.broadcasted_iota(jnp.int32, (blocks, blocks), 1)
    for f in range(freqs):
        packed = gram[f // 2][:, (f % 2) * blocks : (f % 2 + 1) * blocks]
        flipped = packed.T
        real = jnp.where(row <= col, packed, flipped)
        imag = jnp.where(row > col, packed, jnp.where(row < col, -flipped, 0.0))
        top = jnp.concatenate([real, -imag], axis=1)
        bottom = jnp.concatenate([imag, real], axis=1)
        high, low = split(jnp.concatenate([top, bottom], axis=0))
        mats[f] = jnp.concatenate([high, low], axis=1)

    def apply(vec):
        parts = []
        for f in range(freqs):
            high, low = split(vec[f])
            out = dot_plain(jnp.concatenate([high, low], axis=0), mats[f])
            out = out[:rank] + out[rank:]
            parts.append((out[:, both:] + out[:, :both])[None])
        return jnp.concatenate(parts, axis=0)

    lane = lax.broadcasted_iota(jnp.int32, (1, 1, both), 2)
    sub = lax.broadcasted_iota(jnp.int32, (1, rank, 1), 1)
    sign = jnp.where(lane < blocks, -1.0, 1.0).astype(F32)

    def orthonormalize(z):
        turned = pltpu.roll(z.reshape(freqs * rank, both), blocks, 1).reshape(z.shape) * sign
        for k in range(rank):
            base = z[:, k : k + 1, :]
            across = turned[:, k : k + 1, :]
            norm = jnp.sum(base * base, axis=2, keepdims=True) * (1.0 / blocks) + 1e-6
            factor = lax.rsqrt(norm)
            if k + 1 < rank:
                dot_real = jnp.sum(base * z, axis=2, keepdims=True)
                dot_imag = jnp.sum(across * z, axis=2, keepdims=True)
                square = factor * factor * (1.0 / blocks)
                low = jnp.where(sub > k, square, 0.0)
                keep = jnp.where(sub == k, factor, 1.0)
                coef_real = dot_real * low
                coef_imag = dot_imag * low
                z, turned = (
                    z * keep - coef_real * base - coef_imag * across,
                    turned * keep - coef_real * across + coef_imag * base,
                )
            else:
                z = jnp.where(sub == k, z * factor, z)
        return z

    vec = jnp.concatenate([basis[0], basis[1]], axis=2)
    for step in range(ITERS):
        vec = orthonormalize(apply(vec))
    z = apply(vec)
    ray = jnp.sum(vec * z, axis=2, keepdims=True) * (1.0 / blocks)
    total = traces[0][...]
    for line in traces[1:]:
        total = total + line[...]
    energy = jnp.sum(jnp.where(sub == lane, ray, 0.0), axis=1) * (freqs * groups * blocks)
    rates[...] = (energy / total)[:, :rank]
    rate_write = pltpu.make_async_copy(rates, spectrum, out_sems.at[freqs + 1])
    rate_write.start()
    vecs[0] = vec[:, :, :blocks]
    vecs[1] = vec[:, :, blocks:]
    vec_write = pltpu.make_async_copy(vecs, vec_out, out_sems.at[freqs])
    vec_write.start()
    for f in range(freqs):
        v = vec[f] * (1.0 / blocks)
        real_row = jnp.where(lane[0] < blocks, v, -v)
        imag_row = pltpu.roll(v, blocks, 1)
        high, low = split(jnp.concatenate([real_row, imag_row], axis=0))
        coefs[f] = jnp.concatenate(
            [jnp.concatenate([high, high], axis=1), jnp.concatenate([low, jnp.zeros_like(low)], axis=1)], axis=0
        )

    def project(step, carry):
        first = step * TOGETHER
        for f in range(TOGETHER):
            read(first + f).wait()
        for f in range(TOGETHER):
            f = first + f
            coef = coefs[f]
            for c in range(comps):
                x = buf[f, :, c].reshape(both, -1)
                x_high, x_low = split(x)
                out = dot_plain(coef, jnp.concatenate([x_high, x_low], axis=0))
                out = out[: 2 * rank] + out[2 * rank :]
                res[0, f, c] = out[:rank]
                res[1, f, c] = out[rank:]
            write(f).start()
        return carry

    lax.fori_loop(0, freqs // TOGETHER, project, 0)
    for f in range(freqs):
        write(f).wait()
    vec_write.wait()
    rate_write.wait()


def per_device(data, quad_weight, basis):
    _, freqs, blocks, comps, points = data.shape
    rank = basis.shape[-1]
    freq_groups = lax.axis_size("freq")
    size = lax.axis_size("pts")
    freq_count = freqs * freq_groups
    scaling = 1.0 / (comps * points * size)
    pieces = freqs // 2 * blocks // 8
    samples = jnp.transpose(data, (0, 1, 3, 2, 4))
    start = jnp.transpose(basis, (0, 1, 3, 2))
    vmem = pl.BlockSpec(memory_space=pltpu.VMEM)
    hbm = pl.BlockSpec(memory_space=pltpu.MemorySpace.HBM)
    packed = pl.pallas_call(
        lambda *refs: gram_kernel(freqs, blocks, comps, scaling, *refs),
        out_shape=pltpu.VMEM((pieces * 9, 1, 2 * blocks), F32),
        in_specs=[hbm, hbm],
        out_specs=vmem,
        scratch_shapes=[
            pltpu.VMEM((freqs, 2, comps, blocks, points), F32),
            pltpu.VMEM((1, points), F32),
            pltpu.VMEM((freqs, 2 * blocks, 4 * blocks), F32),
            pltpu.SemaphoreType.DMA((freqs + 1 + comps,)),
        ],
        compiler_params=pltpu.CompilerParams(vmem_limit_bytes=60 * 2**20),
        name="gram",
    )(samples, quad_weight.reshape(1, points))
    arrived = lax.all_to_all(packed, "pts", 0, 0, tiled=True)
    spread, trace = pl.pallas_call(
        lambda *refs: sum_kernel(size, *refs),
        out_shape=(
            jax.ShapeDtypeStruct((size, 8, 2 * blocks), F32),
            jax.ShapeDtypeStruct((1, 2 * blocks), F32),
        ),
        in_specs=[vmem],
        out_specs=(vmem, vmem),
        compiler_params=pltpu.CompilerParams(vmem_limit_bytes=2 * 2**20),
        name="total",
    )(arrived)
    others = [
        lax.ppermute(trace, "freq", [(i, (i + d) % freq_groups) for i in range(freq_groups)])
        for d in range(1, freq_groups)
    ]
    gram = lax.all_to_all(spread, "pts", 0, 0, tiled=True).reshape(freqs // 2, blocks, 2 * blocks)
    traces = [trace, *others]
    vec, spectrum, modes = pl.pallas_call(
        lambda *refs: finish_kernel(freqs, blocks, comps, rank, freq_groups, *refs),
        out_shape=(
            jax.ShapeDtypeStruct((2, freqs, rank, blocks), F32),
            jax.ShapeDtypeStruct((freqs, rank), F32),
            jax.ShapeDtypeStruct((2, freqs, comps, rank, points), F32),
        ),
        in_specs=[vmem, vmem, hbm] + [vmem] * freq_groups,
        out_specs=(hbm, hbm, hbm),
        scratch_shapes=[
            pltpu.VMEM((freqs, 2, comps, blocks, points), F32),
            pltpu.VMEM((2, freqs, comps, rank, points), F32),
            pltpu.VMEM((2, freqs, rank, blocks), F32),
            pltpu.VMEM((freqs, rank), F32),
            pltpu.VMEM((freqs, 2 * blocks, 4 * blocks), BF16),
            pltpu.VMEM((freqs, 4 * rank, 4 * blocks), BF16),
            pltpu.SemaphoreType.DMA((freqs,)),
            pltpu.SemaphoreType.DMA((freqs + 2,)),
        ],
        compiler_params=pltpu.CompilerParams(vmem_limit_bytes=52 * 2**20),
        name="finish",
    )(gram, start, samples, *traces)
    return (
        jnp.transpose(vec, (0, 1, 3, 2)),
        spectrum,
        jnp.transpose(modes, (0, 1, 3, 2, 4)),
    )


def solution(mesh):
    in_specs = (P(None, "freq", None, None, "pts"), P("pts"), P(None, "freq", None, None))
    out_specs = (P(None, "freq", None, None), P("freq", None), P(None, "freq", None, None, "pts"))
    return jax.shard_map(
        per_device, mesh=mesh, in_specs=in_specs, out_specs=out_specs, check_vma=False
    )
```

```python
import jax
import jax.numpy as jnp
from jax import lax
from jax.experimental import pallas as pl
from jax.experimental.pallas import tpu as pltpu
from jax.sharding import PartitionSpec as P

ITERS = 4
TOGETHER = 4
F32 = jnp.float32
BF16 = jnp.bfloat16


def split(x):
    high = x.astype(BF16)
    low = (x - high.astype(F32)).astype(BF16)
    return high, low


def dot_rows(left, right):
    return lax.dot_general(left, right, (((1,), (1,)), ((), ())), preferred_element_type=F32)


def dot_plain(left, right):
    return lax.dot_general(left, right, (((1,), (0,)), ((), ())), preferred_element_type=F32)


def gram_kernel(freqs, blocks, comps, scaling, data, weight, out, buf, lines, sums, sems):
    def read(f):
        return pltpu.make_async_copy(data.at[:, f], buf.at[f], sems.at[f])

    weight_read = pltpu.make_async_copy(weight, lines, sems.at[freqs])
    weight_read.start()
    for f in range(freqs):
        read(f).start()
    weight_read.wait()
    root = jnp.sqrt(lines[...])
    row = lax.broadcasted_iota(jnp.int32, (blocks, blocks), 0)
    col = lax.broadcasted_iota(jnp.int32, (blocks, blocks), 1)
    both = 2 * blocks

    def multiply(first, count):
        for f in range(count):
            read(first + f).wait()
        for f in range(count):
            f = first + f
            acc = jnp.zeros((both, 2 * both), F32)
            for c in range(comps):
                x = buf[f, :, c].reshape(both, -1) * root
                high, low = split(x)
                acc = acc + dot_plain(high, jnp.concatenate([high.T, low.T], axis=1))
            sums[f] = acc

    def pack(pair, trace):
        packed = []
        for half in range(2):
            acc = sums[2 * pair + half]
            cross = acc[:, both:]
            full = (acc[:, :both] + (cross + cross.T)) * scaling
            real = full[:blocks, :blocks] + full[blocks:, blocks:]
            imag = full[:blocks, blocks:] - full[blocks:, :blocks]
            packed.append(jnp.where(row <= col, real, imag))
            trace = trace + jnp.where(row == col, real, 0.0)
        wide = jnp.concatenate(packed, axis=1)
        for b in range(blocks // 8):
            for r in range(8):
                out[pair * (blocks // 8) + b, :, both * r : both * (r + 1)] = wide[8 * b + r : 8 * b + r + 1, :]
        return trace

    def pair_step(pair, trace):
        trace = pack(pair - 1, trace)
        multiply(2 * pair, 2)
        return trace

    pairs = freqs // 2
    multiply(0, 1)
    multiply(1, 1)
    trace = jnp.zeros((blocks, blocks), F32)
    for pair in range(1, pairs):
        trace = pair_step(pair, trace)
    trace = pack(pairs - 1, trace)
    value = jnp.sum(jnp.sum(trace, axis=1, keepdims=True), axis=0, keepdims=True)
    line = jnp.broadcast_to(value, (1, both))
    for piece in range(freqs // 2 * blocks // 8):
        out[piece, :, 8 * both :] = line


def sum_kernel(pieces, arrived, out, trace):
    total = arrived[0]
    for p in range(1, pieces):
        total = total + arrived[p]
    width = out.shape[2]
    lines = jnp.concatenate([total[:, width * r : width * (r + 1)] for r in range(8)], axis=0)
    for p in range(pieces):
        out[p] = lines
    trace[...] = total[:, 8 * width :]


def finish_kernel(freqs, blocks, comps, rank, groups, gram, basis, data, *refs):
    traces = refs[:groups]
    vec_out, spectrum, modes, buf, res, vecs, rates, mats, coefs, sems, out_sems = refs[groups:]

    def read(f):
        return pltpu.make_async_copy(data.at[:, f], buf.at[f], sems.at[f])

    def write(f):
        return pltpu.make_async_copy(res.at[:, f], modes.at[:, f], out_sems.at[f])

    for f in range(freqs):
        read(f).start()
    both = 2 * blocks
    row = lax.broadcasted_iota(jnp.int32, (blocks, blocks), 0)
    col = lax.broadcasted_iota(jnp.int32, (blocks, blocks), 1)
    for f in range(freqs):
        packed = gram[f // 2][:, (f % 2) * blocks : (f % 2 + 1) * blocks]
        flipped = packed.T
        real = jnp.where(row <= col, packed, flipped)
        imag = jnp.where(row > col, packed, jnp.where(row < col, -flipped, 0.0))
        top = jnp.concatenate([real, -imag], axis=1)
        bottom = jnp.concatenate([imag, real], axis=1)
        high, low = split(jnp.concatenate([top, bottom], axis=0))
        mats[f] = jnp.concatenate([high, low], axis=1)

    def apply(vec):
        parts = []
        for f in range(freqs):
            high, low = split(vec[f])
            out = dot_plain(jnp.concatenate([high, low], axis=0), mats[f])
            out = out[:rank] + out[rank:]
            parts.append((out[:, both:] + out[:, :both])[None])
        return jnp.concatenate(parts, axis=0)

    lane = lax.broadcasted_iota(jnp.int32, (1, 1, both), 2)
    sub = lax.broadcasted_iota(jnp.int32, (1, rank, 1), 1)
    sign = jnp.where(lane < blocks, -1.0, 1.0).astype(F32)

    def orthonormalize(z):
        turned = pltpu.roll(z.reshape(freqs * rank, both), blocks, 1).reshape(z.shape) * sign
        for k in range(rank):
            base = z[:, k : k + 1, :]
            across = turned[:, k : k + 1, :]
            dot_real = jnp.sum(base * z, axis=2, keepdims=True)
            norm = dot_real[:, k : k + 1, :] * (1.0 / blocks) + 1e-6
            factor = lax.rsqrt(norm)
            if k + 1 < rank:
                dot_imag = jnp.sum(across * z, axis=2, keepdims=True)
                square = factor * factor * (1.0 / blocks)
                low = jnp.where(sub > k, square, 0.0)
                keep = jnp.where(sub == k, factor, 1.0)
                coef_real = dot_real * low
                coef_imag = dot_imag * low
                z, turned = (
                    z * keep - coef_real * base - coef_imag * across,
                    turned * keep - coef_real * across + coef_imag * base,
                )
            else:
                z = jnp.where(sub == k, z * factor, z)
        return z

    vec = jnp.concatenate([basis[0], basis[1]], axis=2)
    for step in range(ITERS):
        vec = orthonormalize(apply(vec))
    z = apply(vec)
    ray = jnp.sum(vec * z, axis=2, keepdims=True) * (1.0 / blocks)
    total = traces[0][...]
    for line in traces[1:]:
        total = total + line[...]
    energy = jnp.sum(jnp.where(sub == lane, ray, 0.0), axis=1) * (freqs * groups * blocks)
    rates[...] = (energy / total)[:, :rank]
    rate_write = pltpu.make_async_copy(rates, spectrum, out_sems.at[freqs + 1])
    rate_write.start()
    vecs[0] = vec[:, :, :blocks]
    vecs[1] = vec[:, :, blocks:]
    vec_write = pltpu.make_async_copy(vecs, vec_out, out_sems.at[freqs])
    vec_write.start()
    for f in range(freqs):
        v = vec[f] * (1.0 / blocks)
        real_row = jnp.where(lane[0] < blocks, v, -v)
        imag_row = pltpu.roll(v, blocks, 1)
        high, low = split(jnp.concatenate([real_row, imag_row], axis=0))
        coefs[f] = jnp.concatenate(
            [jnp.concatenate([high, high], axis=1), jnp.concatenate([low, jnp.zeros_like(low)], axis=1)], axis=0
        )

    def project(step, carry):
        first = step * TOGETHER
        for f in range(TOGETHER):
            read(first + f).wait()
        for f in range(TOGETHER):
            f = first + f
            coef = coefs[f]
            for c in range(comps):
                x = buf[f, :, c].reshape(both, -1)
                x_high, x_low = split(x)
                out = dot_plain(coef, jnp.concatenate([x_high, x_low], axis=0))
                out = out[: 2 * rank] + out[2 * rank :]
                res[0, f, c] = out[:rank]
                res[1, f, c] = out[rank:]
            write(f).start()
        return carry

    lax.fori_loop(0, freqs // TOGETHER, project, 0)
    for f in range(freqs):
        write(f).wait()
    vec_write.wait()
    rate_write.wait()


def per_device(data, quad_weight, basis):
    _, freqs, blocks, comps, points = data.shape
    rank = basis.shape[-1]
    freq_groups = lax.axis_size("freq")
    size = lax.axis_size("pts")
    freq_count = freqs * freq_groups
    scaling = 1.0 / (comps * points * size)
    pieces = freqs // 2 * blocks // 8
    samples = jnp.transpose(data, (0, 1, 3, 2, 4))
    start = jnp.transpose(basis, (0, 1, 3, 2))
    vmem = pl.BlockSpec(memory_space=pltpu.VMEM)
    hbm = pl.BlockSpec(memory_space=pltpu.MemorySpace.HBM)
    packed = pl.pallas_call(
        lambda *refs: gram_kernel(freqs, blocks, comps, scaling, *refs),
        out_shape=pltpu.VMEM((pieces, 1, 18 * blocks), F32),
        in_specs=[hbm, hbm],
        out_specs=vmem,
        scratch_shapes=[
            pltpu.VMEM((freqs, 2, comps, blocks, points), F32),
            pltpu.VMEM((1, points), F32),
            pltpu.VMEM((freqs, 2 * blocks, 4 * blocks), F32),
            pltpu.SemaphoreType.DMA((freqs + 1,)),
        ],
        compiler_params=pltpu.CompilerParams(vmem_limit_bytes=60 * 2**20),
        name="gram",
    )(samples, quad_weight.reshape(1, points))
    arrived = lax.all_to_all(packed, "pts", 0, 0, tiled=True)
    spread, trace = pl.pallas_call(
        lambda *refs: sum_kernel(size, *refs),
        out_shape=(
            jax.ShapeDtypeStruct((size, 8, 2 * blocks), F32),
            jax.ShapeDtypeStruct((1, 2 * blocks), F32),
        ),
        in_specs=[vmem],
        out_specs=(vmem, vmem),
        compiler_params=pltpu.CompilerParams(vmem_limit_bytes=2 * 2**20),
        name="total",
    )(arrived)
    others = [
        lax.ppermute(trace, "freq", [(i, (i + d) % freq_groups) for i in range(freq_groups)])
        for d in range(1, freq_groups)
    ]
    gram = lax.all_to_all(spread, "pts", 0, 0, tiled=True).reshape(freqs // 2, blocks, 2 * blocks)
    traces = [trace, *others]
    vec, spectrum, modes = pl.pallas_call(
        lambda *refs: finish_kernel(freqs, blocks, comps, rank, freq_groups, *refs),
        out_shape=(
            jax.ShapeDtypeStruct((2, freqs, rank, blocks), F32),
            jax.ShapeDtypeStruct((freqs, rank), F32),
            jax.ShapeDtypeStruct((2, freqs, comps, rank, points), F32),
        ),
        in_specs=[vmem, vmem, hbm] + [vmem] * freq_groups,
        out_specs=(hbm, hbm, hbm),
        scratch_shapes=[
            pltpu.VMEM((freqs, 2, comps, blocks, points), F32),
            pltpu.VMEM((2, freqs, comps, rank, points), F32),
            pltpu.VMEM((2, freqs, rank, blocks), F32),
            pltpu.VMEM((freqs, rank), F32),
            pltpu.VMEM((freqs, 2 * blocks, 4 * blocks), BF16),
            pltpu.VMEM((freqs, 4 * rank, 4 * blocks), BF16),
            pltpu.SemaphoreType.DMA((freqs,)),
            pltpu.SemaphoreType.DMA((freqs + 2,)),
        ],
        compiler_params=pltpu.CompilerParams(vmem_limit_bytes=52 * 2**20),
        name="finish",
    )(gram, start, samples, *traces)
    return (
        jnp.transpose(vec, (0, 1, 3, 2)),
        spectrum,
        jnp.transpose(modes, (0, 1, 3, 2, 4)),
    )


def solution(mesh):
    in_specs = (P(None, "freq", None, None, "pts"), P("pts"), P(None, "freq", None, None))
    out_specs = (P(None, "freq", None, None), P("freq", None), P(None, "freq", None, None, "pts"))
    return jax.shard_map(
        per_device, mesh=mesh, in_specs=in_specs, out_specs=out_specs, check_vma=False
    )
```
